8 devices in a mesh: dp: 2 (over y, z), tp: 4 (over x, core).
Axes of the slice: x: 2, y: 2, z: 1, core: 2. Of those that a mesh axis runs over, the one named last changes fastest.
Arguments:
- x: bfloat16 [4096, 2048], P('dp'), parts along dimension 0
- dy: bfloat16 [4096, 2048], P('dp'), parts along dimension 0
- gate: bfloat16 [4096, 5120], P('dp', 'tp'), parts along dimension 0
- up: bfloat16 [4096, 5120], P('dp', 'tp'), parts along dimension 0
- w_gate: bfloat16 [2048, 5120], P(None, 'tp')
- w_up: bfloat16 [2048, 5120], P(None, 'tp')
- w_down: bfloat16 [5120, 2048], P('tp')
Outputs:
- output 1: bfloat16 [4096, 2048], P('dp'), parts along dimension 0
- output 2: bfloat16 [4096, 5120], P('dp', 'tp'), parts along dimension 0
- output 3: bfloat16 [4096, 5120], P('dp', 'tp'), parts along dimension 0
- output 4: bfloat16 [10240, 2048], P(('dp', 'tp')), parts along dimension 0
There are 2 independent parts. The reference program is written for one: setup_inputs(seed, part) draws one part's arguments, and reference() takes and returns one part's arrays. A program takes and returns all parts, laid end to end along the dimension named above; an argument that names none is the same for every part.
All inputs are finite; a program needn't handle non-finite values.
Results may differ from the reference program's by a relative error of at most 0.012.
Values are sent between devices in bfloat16 or wider.
A program may use at most 2 GiB of HBM per device.

```python
import jax
import jax.numpy as jnp

ROWS = 2048
D = 2048
FF = 5120


def act(gate, up):
    return jax.nn.gelu(gate) * up


def setup_inputs(seed: int = 0, part: int = 0) -> dict:
    kx, ky, ka, kb, kg, ku, kd = jax.random.split(jax.random.key(seed), 7)
    kx, ky, ka, kb = (jax.random.fold_in(k, part) for k in (kx, ky, ka, kb))
    drawn = {
        "x": jax.random.normal(kx, (ROWS, D), jnp.float32),
        "dy": jax.random.normal(ky, (ROWS, D), jnp.float32),
        "gate": jax.random.normal(ka, (ROWS, FF), jnp.float32),
        "up": jax.random.normal(kb, (ROWS, FF), jnp.float32),
        "w_gate": jax.random.normal(kg, (D, FF), jnp.float32) * D**-0.5,
        "w_up": jax.random.normal(ku, (D, FF), jnp.float32) * D**-0.5,
        "w_down": jax.random.normal(kd, (FF, D), jnp.float32) * FF**-0.5,
    }
    return {k: v.astype(jnp.bfloat16) for k, v in drawn.items()}


def reference(x, dy, gate, up, w_gate, w_up, w_down):
    hidden, back = jax.vjp(act, gate.astype(jnp.float32), up.astype(jnp.float32))
    d_hidden = jnp.dot(dy, w_down.T, preferred_element_type=jnp.float32)
    d_gate, d_up = (g.astype(jnp.bfloat16) for g in back(d_hidden))
    dx = jnp.dot(d_gate, w_gate.T, preferred_element_type=jnp.float32) + jnp.dot(d_up, w_up.T, preferred_element_type=jnp.float32)
    dw_gate = jnp.dot(x.T, d_gate, preferred_element_type=jnp.float32)
    dw_up = jnp.dot(x.T, d_up, preferred_element_type=jnp.float32)
    dw_down = jnp.dot(hidden.astype(jnp.bfloat16).T, dy, preferred_element_type=jnp.float32)
    return tuple(g.astype(jnp.bfloat16) for g in (dx, dw_gate, dw_up, dw_down))
```

```python
import functools

import jax
import jax.numpy as jnp
from jax import lax
from jax.experimental import pallas as pl
from jax.experimental.pallas import tpu as pltpu
from jax.sharding import PartitionSpec as P

MESH = pl.DeviceIdType.MESH
NT = (((1,), (1,)), ((), ()))
TN = (((0,), (0,)), ((), ()))
BF16, F32 = jnp.bfloat16, jnp.float32

CHUNK = 256
HALF = CHUNK // 2
TILE = 256
LATE = 3
C0 = 0.7978845608028654
C1 = 0.044715


def dot(a, b, dims):
    return lax.dot_general(a, b, dims, preferred_element_type=F32)


def kernel(
    x, dy, gate, up, w_gate, w_up, w_down,
    dx, dw_gate, dw_up, dw_down,
    dy_v, gate_v, up_v, hid_v, got_x, got_c, keep, give, x_v,
    w_sem, in_sem, x_sem, give_sem, got_c_sem, send_x_sem, got_x_sem, fin_sem, got_fin_sem,
):
    rows, d = dx.shape
    ff = dw_gate.shape[1]
    n = rows // CHUNK
    pieces = 2 * n
    cols = d // 2
    me = lax.axis_index("tp")
    core = lax.rem(me, 2)
    mate = me + 1 - 2 * core
    across = lax.rem(me + 2, 4)

    def load(src, dst, sem):
        return pltpu.make_async_copy(src, dst, sem)

    def chunk_loads(c):
        r = pl.ds(pl.multiple_of(c * CHUNK, CHUNK), CHUNK)
        return [
            load(dy.at[r], dy_v.at[r], in_sem.at[0, c]),
            load(gate.at[r], gate_v.at[r], in_sem.at[1, c]),
            load(up.at[r], up_v.at[r], in_sem.at[2, c]),
        ]

    def weight_loads(h):
        r = pl.ds(h * cols, cols)
        return [
            load(w_gate.at[r], dw_gate.at[r], w_sem.at[1 + 2 * h]),
            load(w_up.at[r], dw_up.at[r], w_sem.at[2 + 2 * h]),
        ]

    def x_load(k):
        c = pl.ds(pl.multiple_of(k * TILE, TILE), TILE)
        slot = lax.rem(k, 2)
        return load(x.at[:, c], x_v.at[slot], x_sem.at[slot])

    def to(device):
        return dict(device_id={"tp": device}, device_id_type=MESH)

    def own_rows(c):
        return pl.ds(pl.multiple_of(c * CHUNK + core * HALF, HALF), HALF)

    def piece_of(p):
        c, h = p // 2, lax.rem(p, 2)
        return own_rows(c), pl.ds(pl.multiple_of(h * cols, cols), cols)

    def give_copy(p):
        h = lax.rem(p, 2)
        return pltpu.make_async_remote_copy(
            give.at[h], got_c.at[p], give_sem.at[p], got_c_sem.at[p], **to(mate)
        )

    def cross_copy(p):
        r, c = piece_of(p)
        return pltpu.make_async_remote_copy(
            dx.at[r, c], got_x.at[p], send_x_sem.at[p], got_x_sem.at[p], **to(across)
        )

    def final_copy(p):
        r, c = piece_of(p)
        return pltpu.make_async_remote_copy(
            dx.at[r, c], dx.at[r, c], fin_sem.at[p], got_fin_sem.at[p], **to(mate)
        )

    def add_mate(p, h):
        give_copy(p).wait_recv()
        r, c = piece_of(p)
        dx[r, c] = (keep[h] + got_c[p].astype(F32)).astype(BF16)
        cross_copy(p).start()

    def finish(p):
        cross_copy(p).wait()
        r, c = piece_of(p)
        dx[r, c] = (dx[r, c].astype(F32) + got_x[p].astype(F32)).astype(BF16)
        final_copy(p).start()

    first = chunk_loads(0)
    down = load(w_down, dw_down, w_sem.at[0])
    first[0].start()
    down.start()
    first[1].start()
    first[2].start()
    for h in range(2):
        for w in weight_loads(h):
            w.start()

    barrier = pltpu.get_barrier_semaphore()
    for device in (mate, across):
        pl.semaphore_signal(barrier, inc=1, **to(device))
    pl.semaphore_wait(barrier, 2)

    down.wait()

    @pl.loop(0, n)
    def _(c):
        for w in chunk_loads(c):
            w.wait()

        @pl.when(c + 1 < n)
        def _():
            for w in chunk_loads(c + 1):
                w.start()

        r = pl.ds(pl.multiple_of(c * CHUNK, CHUNK), CHUNK)
        for t in range(ff // TILE):
            f = pl.ds(t * TILE, TILE)
            dh = dot(dy_v[r, :], dw_down[f, :], NT)
            g = gate_v[r, f].astype(F32)
            u = up_v[r, f].astype(F32)
            g2 = g * g
            s = 0.5 + 0.5 * jnp.tanh(g * (C0 + (C0 * C1) * g2))
            gelu = g * s
            slope = s + g * (2.0 * C0 + (6.0 * C0 * C1) * g2) * (s - s * s)
            hid_v[r, f] = (gelu * u).astype(BF16)
            gate_v[r, f] = (dh * u * slope).astype(BF16)
            up_v[r, f] = (dh * gelu).astype(BF16)

        @pl.when(c > 0)
        def _():
            add_mate(2 * c - 1, 1)

        mine = own_rows(c)
        other = pl.ds(pl.multiple_of(c * CHUNK + (1 - core) * HALF, HALF), HALF)
        for h in range(2):
            p = 2 * c + h

            @pl.when(c == 0)
            def _():
                for w in weight_loads(h):
                    w.wait()

            @pl.when(c > 0)
            def _():
                give_copy(p - 2).wait_send()

            lhs = jnp.concatenate(
                [
                    jnp.concatenate([gate_v[mine, :], up_v[mine, :]], axis=1),
                    jnp.concatenate([gate_v[other, :], up_v[other, :]], axis=1),
                ],
                axis=0,
            )
            for t in range(cols // TILE):
                w = pl.ds(h * cols + t * TILE, TILE)
                rhs = jnp.concatenate([dw_gate[w, :], dw_up[w, :]], axis=1)
                term = dot(lhs, rhs, NT)
                keep[h, :, t * TILE : (t + 1) * TILE] = term[:HALF]
                give[h, :, t * TILE : (t + 1) * TILE] = term[HALF:].astype(BF16)
            give_copy(p).start()
            if h == 1:
                add_mate(2 * c, 0)

        @pl.when(c == n - 2)
        def _():
            x_load(0).start()

        @pl.when(c >= LATE)
        def _():
            finish(c - LATE)

    add_mate(pieces - 1, 1)
    for p in (pieces - 2, pieces - 1):
        give_copy(p).wait_send()
    done = n - LATE

    tiles = d // TILE

    @pl.loop(0, tiles)
    def _(k):
        x_load(k).wait()

        @pl.when(k + 1 < tiles)
        def _():
            x_load(k + 1).start()

        r = pl.ds(pl.multiple_of(k * TILE, TILE), TILE)
        slot = lax.rem(k, 2)
        dw_gate[r, :] = dot(x_v[slot], gate_v[...], TN).astype(BF16)
        dw_up[r, :] = dot(x_v[slot], up_v[...], TN).astype(BF16)

        @pl.when(lax.rem(k, 2) == 1)
        def _():
            finish(done + k // 2)

    done += tiles // 2

    @pl.loop(0, ff // TILE)
    def _(k):
        f = pl.ds(pl.multiple_of(k * TILE, TILE), TILE)
        for h in range(2):
            c = pl.ds(h * cols, cols)
            dw_down[f, c] = dot(hid_v[:, f], dy_v[:, c], TN).astype(BF16)

        @pl.when(lax.rem(k, 2) == 1)
        def _():
            finish(done + k // 2)

    done += ff // TILE // 2

    @pl.loop(done, pieces)
    def _(p):
        finish(p)

    @pl.loop(0, pieces)
    def _(p):
        final_copy(p).wait()


def store(*refs):
    n = len(refs) // 2
    copies = [pltpu.make_async_copy(refs[i], refs[n + i], refs[-1].at[i]) for i in range(n)]
    for c in copies:
        c.start()
    for c in copies:
        c.wait()


def backward(x, dy, gate, up, w_gate, w_up, w_down):
    rows, d = x.shape
    ff = gate.shape[1]
    pieces = 2 * rows // CHUNK
    cols = d // 2
    hbm = pl.BlockSpec(memory_space=pl.ANY)
    sem = pltpu.SemaphoreType.DMA
    parts = pl.pallas_call(
        kernel,
        out_shape=tuple(pltpu.VMEM(s, BF16) for s in ((rows, d), (d, ff), (d, ff), (ff, d))),
        in_specs=[hbm] * 7,
        out_specs=(pl.BlockSpec(memory_space=pltpu.VMEM),) * 4,
        scratch_shapes=[
            pltpu.VMEM((rows, d), BF16),
            pltpu.VMEM((rows, ff), BF16),
            pltpu.VMEM((rows, ff), BF16),
            pltpu.VMEM((rows, ff), BF16),
            pltpu.VMEM((pieces, HALF, cols), BF16),
            pltpu.VMEM((pieces, HALF, cols), BF16),
            pltpu.VMEM((2, HALF, cols), F32),
            pltpu.VMEM((2, HALF, cols), BF16),
            pltpu.VMEM((2, rows, TILE), BF16),
            sem((5,)),
            sem((3, rows // CHUNK)),
            sem((2,)),
        ]
        + [sem((pieces,))] * 6,
        compiler_params=pltpu.CompilerParams(
            collective_id=0, has_side_effects=True, vmem_limit_bytes=39 * 2**20
        ),
        cost_estimate=pl.CostEstimate(
            flops=12 * rows * d * ff, bytes_accessed=64 * 2**20, transcendentals=rows * ff
        ),
        name="mlp_backward",
    )(x, dy, gate, up, w_gate, w_up, w_down)
    return pl.pallas_call(
        store,
        out_shape=tuple(pltpu.HBM(p.shape, p.dtype) for p in parts),
        in_specs=[pl.BlockSpec(memory_space=pltpu.VMEM)] * len(parts),
        out_specs=(pl.BlockSpec(memory_space=pltpu.HBM),) * len(parts),
        scratch_shapes=[sem((len(parts),))],
        compiler_params=pltpu.CompilerParams(vmem_limit_bytes=2**20),
        name="store",
    )(*parts)


def solution(mesh):
    tokens, columns, down = P("dp", None), P(None, "tp"), P("tp", None)
    return jax.shard_map(
        backward,
        mesh=mesh,
        in_specs=(tokens, tokens, P("dp", "tp"), P("dp", "tp"), columns, columns, down),
        out_specs=(tokens, P("dp", "tp"), P("dp", "tp"), P(("dp", "tp"), None)),
        check_vma=False,
    )
```

```python
import functools

import jax
import jax.numpy as jnp
from jax import lax
from jax.experimental import pallas as pl
from jax.experimental.pallas import tpu as pltpu
from jax.sharding import PartitionSpec as P

MESH = pl.DeviceIdType.MESH
NT = (((1,), (1,)), ((), ()))
TN = (((0,), (0,)), ((), ()))
BF16, F32 = jnp.bfloat16, jnp.float32

CHUNK = 256
HALF = CHUNK // 2
TILE = 256
PIECE = 512
RING = 8
SPLIT = 4
C0 = 0.7978845608028654
C1 = 0.044715


def dot(a, b, dims):
    return lax.dot_general(a, b, dims, preferred_element_type=F32)


def kernel(
    x, dy, gate, up, w_gate, w_up, w_down,
    dx, dw_gate, dw_up, dw_down,
    dy_v, gate_v, up_v, hid_v, got_x, got_c, keep, give, x_v,
    w_sem, in_sem, x_sem, give_sem, got_c_sem, send_x_sem, got_x_sem, fin_sem, got_fin_sem,
):
    rows, d = dx.shape
    ff = dw_gate.shape[1]
    n = rows // CHUNK
    per = d // PIECE
    pieces = per * n
    downs = [(0, 2), (2, 5)]
    last = n - 1
    me = lax.axis_index("tp")
    core = lax.rem(me, 2)
    mate = me + 1 - 2 * core
    across = lax.rem(me + 2, 4)

    def load(src, dst, sem):
        return pltpu.make_async_copy(src, dst, sem)

    def chunk_loads(c):
        r = pl.ds(pl.multiple_of(c * CHUNK, CHUNK), CHUNK)
        return [
            load(dy.at[r], dy_v.at[r], in_sem.at[0, lax.rem(c, 2)]),
            load(gate.at[r], gate_v.at[r], in_sem.at[1, lax.rem(c, 2)]),
            load(up.at[r], up_v.at[r], in_sem.at[2, lax.rem(c, 2)]),
        ]

    def weight_loads(j):
        r = pl.ds(j * PIECE, PIECE)
        return [
            load(w_gate.at[r], dw_gate.at[r], w_sem.at[0, j]),
            load(w_up.at[r], dw_up.at[r], w_sem.at[1, j]),
        ]

    def down_load(b):
        lo, hi = downs[b]
        r = pl.ds(lo * TILE, (hi - lo) * TILE)
        return load(w_down.at[r], dw_down.at[r], w_sem.at[2, b])

    def x_load(k):
        c = pl.ds(pl.multiple_of(k * TILE, TILE), TILE)
        slot = lax.rem(k, 2)
        return load(x.at[:, c], x_v.at[slot], x_sem.at[slot])

    def to(device):
        return dict(device_id={"tp": device}, device_id_type=MESH)

    def own_rows(c):
        return pl.ds(pl.multiple_of(c * CHUNK + core * HALF, HALF), HALF)

    def piece_of(p):
        c, j = p // per, lax.rem(p, per)
        return own_rows(c), pl.ds(pl.multiple_of(j * PIECE, PIECE), PIECE)

    def give_copy(p):
        return pltpu.make_async_remote_copy(
            give.at[lax.rem(p, per)],
            got_c.at[p],
            give_sem.at[lax.rem(p, per)],
            got_c_sem.at[lax.rem(p, RING)],
            **to(mate),
        )

    def cross(refs, slot):
        return pltpu.make_async_remote_copy(
            got_c.at[refs], got_x.at[refs], send_x_sem, got_x_sem.at[slot], **to(across)
        )

    def final_copy(r, c):
        return pltpu.make_async_remote_copy(
            dx.at[r, c], dx.at[r, c], fin_sem, got_fin_sem, **to(mate)
        )

    def add_mate(p):
        give_copy(p).wait_recv()
        got_c[p] = (keep[lax.rem(p, per)] + got_c[p].astype(F32)).astype(BF16)
        slot = jnp.where(p < last * per, p // per, p - last * (per - 1))
        cross(pl.ds(p, 1), slot).start()

    def whole_sum(p):
        r, c = piece_of(p)
        dx[r, c] = (got_c[p].astype(F32) + got_x[p].astype(F32)).astype(BF16)

    def finish_chunk(c):
        cross(pl.ds(pl.multiple_of(c * per, per), per), c).wait_recv()
        for j in range(per):
            whole_sum(c * per + j)
        final_copy(own_rows(c), pl.ds(0, d)).start()

    def finish_last(j):
        p = last * per + j
        cross(pl.ds(p, 1), last + j).wait_recv()
        whole_sum(p)
        final_copy(*piece_of(p)).start()

    def hidden(r, lo, hi):
        for t in range(lo, hi):
            f = pl.ds(t * TILE, TILE)
            dh = dot(dy_v[r, :], dw_down[f, :], NT)
            g = gate_v[r, f].astype(F32)
            u = up_v[r, f].astype(F32)
            g2 = g * g
            s = 0.5 + 0.5 * jnp.tanh(g * (C0 + (C0 * C1) * g2))
            gelu = g * s
            slope = s + g * (2.0 * C0 + (6.0 * C0 * C1) * g2) * (s - s * s)
            hid_v[r, f] = (gelu * u).astype(BF16)
            gate_v[r, f] = (dh * u * slope).astype(BF16)
            up_v[r, f] = (dh * gelu).astype(BF16)

    first = chunk_loads(0)
    first[0].start()
    down_load(0).start()
    first[1].start()
    first[2].start()
    for b in range(1, len(downs)):
        down_load(b).start()

    barrier = pltpu.get_barrier_semaphore()
    for device in (mate, across):
        pl.semaphore_signal(barrier, inc=1, **to(device))

    @pl.loop(0, n)
    def _(c):
        for w in chunk_loads(c):
            w.wait()

        r = pl.ds(pl.multiple_of(c * CHUNK, CHUNK), CHUNK)

        @pl.when(c == 0)
        def _():
            for b, (lo, hi) in enumerate(downs):
                down_load(b).wait()
                for j in range(per * b // len(downs), per * (b + 1) // len(downs)):
                    for w in weight_loads(j):
                        w.start()
                hidden(r, lo, hi)
            pl.semaphore_wait(barrier, 2)

        @pl.when(c > 0)
        def _():
            hidden(r, 0, ff // TILE)

        @pl.when(c + 1 < n)
        def _():
            for w in chunk_loads(c + 1):
                w.start()

        @pl.when(c > 1)
        def _():
            add_mate(per * c - 2)

        @pl.when(c > 0)
        def _():
            add_mate(per * c - 1)

        mine = own_rows(c)
        other = pl.ds(pl.multiple_of(c * CHUNK + (1 - core) * HALF, HALF), HALF)
        for j in range(per):
            p = per * c + j

            @pl.when(c == 0)
            def _():
                for w in weight_loads(j):
                    w.wait()

            @pl.when(c > 0)
            def _():
                give_copy(p - per).wait_send()

            lhs = jnp.concatenate(
                [
                    jnp.concatenate([gate_v[mine, :], up_v[mine, :]], axis=1),
                    jnp.concatenate([gate_v[other, :], up_v[other, :]], axis=1),
                ],
                axis=0,
            )
            for t in range(PIECE // TILE):
                w = pl.ds(j * PIECE + t * TILE, TILE)
                rhs = jnp.concatenate([dw_gate[w, :], dw_up[w, :]], axis=1)
                term = dot(lhs, rhs, NT)
                keep[j, :, t * TILE : (t + 1) * TILE] = term[:HALF]
                give[j, :, t * TILE : (t + 1) * TILE] = term[HALF:].astype(BF16)
            give_copy(p).start()

            if j > 0:

                @pl.when(c == 0)
                def _():
                    add_mate(p - 1)

            if j > 1:

                @pl.when(c > 0)
                def _():
                    add_mate(p - 2)

        @pl.when(c == n - 2)
        def _():
            x_load(0).start()

        @pl.when((c > 2) & (lax.rem(c, 2) == 1))
        def _():
            finish_chunk((c - 3) // 2)

    for p in (pieces - 2, pieces - 1):
        add_mate(p)
    for p in range(pieces - per, pieces):
        give_copy(p).wait_send()
    tiles = d // TILE

    @pl.loop(0, tiles)
    def _(k):
        x_load(k).wait()

        @pl.when(k + 1 < tiles)
        def _():
            x_load(k + 1).start()

        r = pl.ds(pl.multiple_of(k * TILE, TILE), TILE)
        slot = lax.rem(k, 2)
        dw_gate[r, :] = dot(x_v[slot], gate_v[...], TN).astype(BF16)
        dw_up[r, :] = dot(x_v[slot], up_v[...], TN).astype(BF16)
        @pl.when(lax.rem(k, 4) == 1)
        def _():
            finish_chunk(3 + k // 4)

    @pl.loop(0, ff // TILE)
    def _(k):
        f = pl.ds(pl.multiple_of(k * TILE, TILE), TILE)
        for h in range(2):
            c = pl.ds(h * (d // 2), d // 2)
            dw_down[f, c] = dot(hid_v[:, f], dy_v[:, c], TN).astype(BF16)

        @pl.when(k == 1)
        def _():
            finish_chunk(5)

    finish_chunk(6)
    for j in range(per):
        finish_last(j)

    total = pltpu.make_async_remote_copy(got_c, got_x, send_x_sem, got_fin_sem, **to(across))
    total.wait_send()
    total = pltpu.make_async_remote_copy(got_x, got_x, fin_sem, got_fin_sem, **to(mate))
    total.wait()


def store(*refs):
    n = len(refs) // 2
    copies = []
    for i in range(n):
        step = refs[i].shape[0] // SPLIT
        for k in range(SPLIT):
            r = pl.ds(k * step, step)
            copies.append(pltpu.make_async_copy(refs[i].at[r], refs[n + i].at[r], refs[-1].at[i, k]))
    for c in copies:
        c.start()
    for c in copies:
        c.wait()


def backward(x, dy, gate, up, w_gate, w_up, w_down):
    rows, d = x.shape
    ff = gate.shape[1]
    per = d // PIECE
    pieces = per * rows // CHUNK
    hbm = pl.BlockSpec(memory_space=pl.ANY)
    sem = pltpu.SemaphoreType.DMA
    parts = pl.pallas_call(
        kernel,
        out_shape=tuple(pltpu.VMEM(s, BF16) for s in ((rows, d), (d, ff), (d, ff), (ff, d))),
        in_specs=[hbm] * 7,
        out_specs=(pl.BlockSpec(memory_space=pltpu.VMEM),) * 4,
        scratch_shapes=[
            pltpu.VMEM((rows, d), BF16),
            pltpu.VMEM((rows, ff), BF16),
            pltpu.VMEM((rows, ff), BF16),
            pltpu.VMEM((rows, ff), BF16),
            pltpu.VMEM((pieces, HALF, PIECE), BF16),
            pltpu.VMEM((pieces, HALF, PIECE), BF16),
            pltpu.VMEM((per, HALF, PIECE), F32),
            pltpu.VMEM((per, HALF, PIECE), BF16),
            pltpu.VMEM((2, rows, TILE), BF16),
            sem((3, per)),
            sem((3, 2)),
            sem((2,)),
            sem((per,)),
            sem((RING,)),
            sem,
            sem((rows // CHUNK - 1 + per,)),
            sem,
            sem,
        ],
        compiler_params=pltpu.CompilerParams(
            collective_id=0, has_side_effects=True, vmem_limit_bytes=39 * 2**20
        ),
        cost_estimate=pl.CostEstimate(
            flops=12 * rows * d * ff, bytes_accessed=64 * 2**20, transcendentals=rows * ff
        ),
        name="mlp_backward",
    )(x, dy, gate, up, w_gate, w_up, w_down)
    return pl.pallas_call(
        store,
        out_shape=tuple(pltpu.HBM(p.shape, p.dtype) for p in parts),
        in_specs=[pl.BlockSpec(memory_space=pltpu.VMEM)] * len(parts),
        out_specs=(pl.BlockSpec(memory_space=pltpu.HBM),) * len(parts),
        scratch_shapes=[sem((len(parts), SPLIT))],
        compiler_params=pltpu.CompilerParams(vmem_limit_bytes=2**20),
        name="store",
    )(*parts)


def solution(mesh):
    tokens, columns, down = P("dp", None), P(None, "tp"), P("tp", None)
    return jax.shard_map(
        backward,
        mesh=mesh,
        in_specs=(tokens, tokens, P("dp", "tp"), P("dp", "tp"), columns, columns, down),
        out_specs=(tokens, P("dp", "tp"), P("dp", "tp"), P(("dp", "tp"), None)),
        check_vma=False,
    )
```

```python
import functools

import jax
import jax.numpy as jnp
from jax import lax
from jax.experimental import pallas as pl
from jax.experimental.pallas import tpu as pltpu
from jax.sharding import PartitionSpec as P

MESH = pl.DeviceIdType.MESH
NT = (((1,), (1,)), ((), ()))
TN = (((0,), (0,)), ((), ()))
BF16, F32 = jnp.bfloat16, jnp.float32

CHUNK = 256
HALF = CHUNK // 2
TILE = 256
PIECE = 512
RING = 6
SPLIT = 2
C0 = 0.7978845608028654
C1 = 0.044715


def dot(a, b, dims):
    return lax.dot_general(a, b, dims, preferred_element_type=F32)


def kernel(
    x, dy, gate, up, w_gate, w_up, w_down,
    dx, dw_gate, dw_up, dw_down,
    dy_v, gate_v, up_v, hid_v, got_x, got_c, keep, give, x_v,
    w_sem, in_sem, x_sem, give_sem, got_c_sem, send_x_sem, got_x_sem, fin_sem, got_fin_sem,
):
    rows, d = dx.shape
    ff = dw_gate.shape[1]
    n = rows // CHUNK
    per = d // PIECE
    pieces = per * n
    downs = [(0, 1), (1, 3), (3, 5)]
    last = n - 1
    me = lax.axis_index("tp")
    core = lax.rem(me, 2)
    mate = me + 1 - 2 * core
    across = lax.rem(me + 2, 4)

    def load(src, dst, sem):
        return pltpu.make_async_copy(src, dst, sem)

    def chunk_loads(c):
        r = pl.ds(pl.multiple_of(c * CHUNK, CHUNK), CHUNK)
        return [
            load(dy.at[r], dy_v.at[r], in_sem.at[0, lax.rem(c, 2)]),
            load(gate.at[r], gate_v.at[r], in_sem.at[1, lax.rem(c, 2)]),
            load(up.at[r], up_v.at[r], in_sem.at[2, lax.rem(c, 2)]),
        ]

    def weight_loads(j):
        r = pl.ds(j * PIECE, PIECE)
        return [
            load(w_gate.at[r], dw_gate.at[r], w_sem.at[0, j]),
            load(w_up.at[r], dw_up.at[r], w_sem.at[1, j]),
        ]

    def down_load(b):
        lo, hi = downs[b]
        r = pl.ds(lo * TILE, (hi - lo) * TILE)
        return load(w_down.at[r], dw_down.at[r], w_sem.at[2, b])

    def x_load(k):
        c = pl.ds(pl.multiple_of(k * TILE, TILE), TILE)
        slot = lax.rem(k, 2)
        return load(x.at[:, c], x_v.at[slot], x_sem.at[slot])

    def to(device):
        return dict(device_id={"tp": device}, device_id_type=MESH)

    def own_rows(c):
        return pl.ds(pl.multiple_of(c * CHUNK + core * HALF, HALF), HALF)

    def piece_of(p):
        c, j = p // per, lax.rem(p, per)
        return own_rows(c), pl.ds(pl.multiple_of(j * PIECE, PIECE), PIECE)

    def give_copy(p):
        return pltpu.make_async_remote_copy(
            give.at[lax.rem(p, per)],
            got_c.at[p],
            give_sem.at[lax.rem(p, per)],
            got_c_sem.at[lax.rem(p, RING)],
            **to(mate),
        )

    def cross(refs, slot):
        return pltpu.make_async_remote_copy(
            got_c.at[refs], got_x.at[refs], send_x_sem, got_x_sem.at[slot], **to(across)
        )

    def final_copy(r, c):
        return pltpu.make_async_remote_copy(
            dx.at[r, c], dx.at[r, c], fin_sem, got_fin_sem, **to(mate)
        )

    def add_mate(p):
        give_copy(p).wait_recv()
        got_c[p] = (keep[lax.rem(p, per)] + got_c[p].astype(F32)).astype(BF16)
        slot = jnp.where(p < last * per, p // per, p - last * (per - 1))
        cross(pl.ds(p, 1), slot).start()

    def whole_sum(p):
        r, c = piece_of(p)
        dx[r, c] = (got_c[p].astype(F32) + got_x[p].astype(F32)).astype(BF16)

    def finish_chunk(c):
        cross(pl.ds(pl.multiple_of(c * per, per), per), c).wait_recv()
        for j in range(per):
            whole_sum(c * per + j)
        final_copy(own_rows(c), pl.ds(0, d)).start()

    def finish_last(j):
        p = last * per + j
        cross(pl.ds(p, 1), last + j).wait_recv()
        whole_sum(p)
        final_copy(*piece_of(p)).start()

    def hidden(r, lo, hi):
        for t in range(lo, hi):
            f = pl.ds(t * TILE, TILE)
            dh = dot(dy_v[r, :], dw_down[f, :], NT)
            g = gate_v[r, f].astype(F32)
            u = up_v[r, f].astype(F32)
            g2 = g * g
            s = 0.5 + 0.5 * jnp.tanh(g * (C0 + (C0 * C1) * g2))
            gelu = g * s
            slope = s + (g * (s * (1.0 - s))) * (2.0 * C0 + (6.0 * C0 * C1) * g2)
            hid_v[r, f] = (gelu * u).astype(BF16)
            gate_v[r, f] = (dh * u * slope).astype(BF16)
            up_v[r, f] = (dh * gelu).astype(BF16)

    first = chunk_loads(0)
    first[0].start()
    down_load(0).start()
    first[1].start()
    first[2].start()
    for b in range(1, len(downs)):
        down_load(b).start(priority=1)

    barrier = pltpu.get_barrier_semaphore()
    for device in (mate, across):
        pl.semaphore_signal(barrier, inc=1, **to(device))

    @pl.loop(0, n)
    def _(c):
        for w in chunk_loads(c):
            w.wait()

        r = pl.ds(pl.multiple_of(c * CHUNK, CHUNK), CHUNK)

        @pl.when(c == 0)
        def _():
            for b, (lo, hi) in enumerate(downs):
                down_load(b).wait()
                for j in range(per * b // len(downs), per * (b + 1) // len(downs)):
                    for w in weight_loads(j):
                        w.start()
                hidden(r, lo, hi)
            pl.semaphore_wait(barrier, 2)

        @pl.when(c > 0)
        def _():
            hidden(r, 0, ff // TILE)

        @pl.when(c + 1 < n)
        def _():
            for w in chunk_loads(c + 1):
                w.start()

        @pl.when(c > 1)
        def _():
            add_mate(per * c - 2)

        @pl.when(c > 0)
        def _():
            add_mate(per * c - 1)

        mine = own_rows(c)
        other = pl.ds(pl.multiple_of(c * CHUNK + (1 - core) * HALF, HALF), HALF)
        for j in range(per):
            p = per * c + j

            @pl.when(c == 0)
            def _():
                for w in weight_loads(j):
                    w.wait()

            @pl.when(c > 0)
            def _():
                give_copy(p - per).wait_send()

            lhs = jnp.concatenate(
                [
                    jnp.concatenate([gate_v[mine, :], up_v[mine, :]], axis=1),
                    jnp.concatenate([gate_v[other, :], up_v[other, :]], axis=1),
                ],
                axis=0,
            )
            for t in range(PIECE // TILE):
                w = pl.ds(j * PIECE + t * TILE, TILE)
                rhs = jnp.concatenate([dw_gate[w, :], dw_up[w, :]], axis=1)
                term = dot(lhs, rhs, NT)
                keep[j, :, t * TILE : (t + 1) * TILE] = term[:HALF]
                give[j, :, t * TILE : (t + 1) * TILE] = term[HALF:].astype(BF16)
            give_copy(p).start()

            if j > 0:

                @pl.when(c == 0)
                def _():
                    add_mate(p - 1)

            if j > 1:

                @pl.when(c > 0)
                def _():
                    add_mate(p - 2)

        @pl.when(c == n - 2)
        def _():
            x_load(0).start()

        @pl.when((c > 2) & (lax.rem(c, 2) == 1))
        def _():
            finish_chunk((c - 3) // 2)

    for p in (pieces - 2, pieces - 1):
        add_mate(p)
    for p in range(pieces - per, pieces):
        give_copy(p).wait_send()
    tiles = d // TILE

    @pl.loop(0, tiles)
    def _(k):
        x_load(k).wait()

        @pl.when(k + 1 < tiles)
        def _():
            x_load(k + 1).start()

        r = pl.ds(pl.multiple_of(k * TILE, TILE), TILE)
        slot = lax.rem(k, 2)
        dw_gate[r, :] = dot(x_v[slot], gate_v[...], TN).astype(BF16)
        dw_up[r, :] = dot(x_v[slot], up_v[...], TN).astype(BF16)
        @pl.when(lax.rem(k, 4) == 1)
        def _():
            finish_chunk(3 + k // 4)

    @pl.loop(0, ff // TILE)
    def _(k):
        f = pl.ds(pl.multiple_of(k * TILE, TILE), TILE)
        for h in range(2):
            c = pl.ds(h * (d // 2), d // 2)
            dw_down[f, c] = dot(hid_v[:, f], dy_v[:, c], TN).astype(BF16)

        @pl.when(k == 1)
        def _():
            finish_chunk(5)

    finish_chunk(6)
    for j in range(per):
        finish_last(j)

    total = pltpu.make_async_remote_copy(got_c, got_x, send_x_sem, got_fin_sem, **to(across))
    total.wait_send()
    total = pltpu.make_async_remote_copy(got_x, got_x, fin_sem, got_fin_sem, **to(mate))
    total.wait()


def store(*refs):
    n = len(refs) // 2
    copies = []
    for i in range(n):
        step = refs[i].shape[0] // SPLIT
        for k in range(SPLIT):
            r = pl.ds(k * step, step)
            copies.append(pltpu.make_async_copy(refs[i].at[r], refs[n + i].at[r], refs[-1].at[i, k]))
    for c in copies:
        c.start()
    for c in copies:
        c.wait()


def backward(x, dy, gate, up, w_gate, w_up, w_down):
    rows, d = x.shape
    ff = gate.shape[1]
    per = d // PIECE
    pieces = per * rows // CHUNK
    hbm = pl.BlockSpec(memory_space=pl.ANY)
    sem = pltpu.SemaphoreType.DMA
    parts = pl.pallas_call(
        kernel,
        out_shape=tuple(pltpu.VMEM(s, BF16) for s in ((rows, d), (d, ff), (d, ff), (ff, d))),
        in_specs=[hbm] * 7,
        out_specs=(pl.BlockSpec(memory_space=pltpu.VMEM),) * 4,
        scratch_shapes=[
            pltpu.VMEM((rows, d), BF16),
            pltpu.VMEM((rows, ff), BF16),
            pltpu.VMEM((rows, ff), BF16),
            pltpu.VMEM((rows, ff), BF16),
            pltpu.VMEM((pieces, HALF, PIECE), BF16),
            pltpu.VMEM((pieces, HALF, PIECE), BF16),
            pltpu.VMEM((per, HALF, PIECE), F32),
            pltpu.VMEM((per, HALF, PIECE), BF16),
            pltpu.VMEM((2, rows, TILE), BF16),
            sem((3, per)),
            sem((3, 2)),
            sem((2,)),
            sem((per,)),
            sem((RING,)),
            sem,
            sem((rows // CHUNK - 1 + per,)),
            sem,
            sem,
        ],
        compiler_params=pltpu.CompilerParams(
            collective_id=0, has_side_effects=True, vmem_limit_bytes=39 * 2**20
        ),
        cost_estimate=pl.CostEstimate(
            flops=12 * rows * d * ff, bytes_accessed=64 * 2**20, transcendentals=rows * ff
        ),
        name="mlp_backward",
    )(x, dy, gate, up, w_gate, w_up, w_down)
    return pl.pallas_call(
        store,
        out_shape=tuple(pltpu.HBM(p.shape, p.dtype) for p in parts),
        in_specs=[pl.BlockSpec(memory_space=pltpu.VMEM)] * len(parts),
        out_specs=(pl.BlockSpec(memory_space=pltpu.HBM),) * len(parts),
        scratch_shapes=[sem((len(parts), SPLIT))],
        compiler_params=pltpu.CompilerParams(vmem_limit_bytes=2**20),
        name="store",
    )(*parts)


def solution(mesh):
    tokens, columns, down = P("dp", None), P(None, "tp"), P("tp", None)
    return jax.shard_map(
        backward,
        mesh=mesh,
        in_specs=(tokens, tokens, P("dp", "tp"), P("dp", "tp"), columns, columns, down),
        out_specs=(tokens, P("dp", "tp"), P("dp", "tp"), P(("dp", "tp"), None)),
        check_vma=False,
    )
```

```python
import functools

import jax
import jax.numpy as jnp
from jax import lax
from jax.experimental import pallas as pl
from jax.experimental.pallas import tpu as pltpu
from jax.sharding import PartitionSpec as P

MESH = pl.DeviceIdType.MESH
NT = (((1,), (1,)), ((), ()))
TN = (((0,), (0,)), ((), ()))
BF16, F32 = jnp.bfloat16, jnp.float32

CHUNK = 256
HALF = CHUNK // 2
TILE = 256
PIECE = 512
RING = 6
SPLIT = 2
C0 = 0.7978845608028654
C1 = 0.044715


def dot(a, b, dims):
    return lax.dot_general(a, b, dims, preferred_element_type=F32)


def kernel(
    x, dy, gate, up, w_gate, w_up, w_down,
    dx, dw_gate, dw_up, dw_down,
    dy_v, gate_v, up_v, hid_v, got_x, got_c, keep, give, x_v,
    w_sem, in_sem, x_sem, give_sem, got_c_sem, send_x_sem, got_x_sem, fin_sem, got_fin_sem,
):
    rows, d = dx.shape
    ff = dw_gate.shape[1]
    n = rows // CHUNK
    per = d // PIECE
    pieces = per * n
    downs = [(0, 1), (1, 3), (3, 5)]
    last = n - 1
    me = lax.axis_index("tp")
    core = lax.rem(me, 2)
    mate = me + 1 - 2 * core
    across = lax.rem(me + 2, 4)

    def load(src, dst, sem):
        return pltpu.make_async_copy(src, dst, sem)

    def chunk_loads(c):
        r = pl.ds(pl.multiple_of(c * CHUNK, CHUNK), CHUNK)
        return [
            load(dy.at[r], dy_v.at[r], in_sem.at[0, lax.rem(c, 2)]),
            load(gate.at[r], gate_v.at[r], in_sem.at[1, lax.rem(c, 2)]),
            load(up.at[r], up_v.at[r], in_sem.at[2, lax.rem(c, 2)]),
        ]

    def weight_loads(j):
        r = pl.ds(j * PIECE, PIECE)
        return [
            load(w_gate.at[r], dw_gate.at[r], w_sem.at[0, j]),
            load(w_up.at[r], dw_up.at[r], w_sem.at[1, j]),
        ]

    def half_loads(t):
        r = pl.ds(t * TILE, TILE)
        return [
            load(w_gate.at[r], dw_gate.at[r], w_sem.at[3 * t, 0]),
            load(w_up.at[r], dw_up.at[r], w_sem.at[1 + 2 * t, t]),
        ]

    def down_load(b):
        lo, hi = downs[b]
        r = pl.ds(lo * TILE, (hi - lo) * TILE)
        return load(w_down.at[r], dw_down.at[r], w_sem.at[2, b])

    def x_load(k):
        c = pl.ds(pl.multiple_of(k * TILE, TILE), TILE)
        slot = lax.rem(k, 2)
        return load(x.at[:, c], x_v.at[slot], x_sem.at[slot])

    def to(device):
        return dict(device_id={"tp": device}, device_id_type=MESH)

    def own_rows(c):
        return pl.ds(pl.multiple_of(c * CHUNK + core * HALF, HALF), HALF)

    def piece_of(p):
        c, j = p // per, lax.rem(p, per)
        return own_rows(c), pl.ds(pl.multiple_of(j * PIECE, PIECE), PIECE)

    def give_copy(p):
        return pltpu.make_async_remote_copy(
            give.at[lax.rem(p, per)],
            got_c.at[p],
            give_sem.at[lax.rem(p, per)],
            got_c_sem.at[lax.rem(p, RING)],
            **to(mate),
        )

    def cross(refs, slot):
        return pltpu.make_async_remote_copy(
            got_c.at[refs], got_x.at[refs], send_x_sem, got_x_sem.at[slot], **to(across)
        )

    def final_copy(r, c):
        return pltpu.make_async_remote_copy(
            dx.at[r, c], dx.at[r, c], fin_sem, got_fin_sem, **to(mate)
        )

    def add_mate(p):
        give_copy(p).wait_recv()
        got_c[p] = (keep[lax.rem(p, per)] + got_c[p].astype(F32)).astype(BF16)
        slot = jnp.where(p < last * per, p // per, p - last * (per - 1))
        cross(pl.ds(p, 1), slot).start()

    def half(t):
        f = pl.ds(t * TILE, TILE)
        swap = pltpu.make_async_remote_copy(
            give.at[0, :, f], got_c.at[0, :, f], give_sem.at[0], got_c_sem.at[t * RING], **to(mate)
        )
        away = pltpu.make_async_remote_copy(
            got_c.at[0, :, f], got_x.at[0, :, f], send_x_sem, got_x_sem.at[0], **to(across)
        )
        return f, swap, away

    def add_half(t):
        f, swap, away = half(t)
        swap.wait_recv()
        got_c[0, :, f] = (keep[0, :, f] + got_c[0, :, f].astype(F32)).astype(BF16)
        away.start()

    def whole_sum(p):
        r, c = piece_of(p)
        dx[r, c] = (got_c[p].astype(F32) + got_x[p].astype(F32)).astype(BF16)

    def finish_chunk(c):
        cross(pl.ds(pl.multiple_of(c * per, per), per), c).wait_recv()
        for j in range(per):
            whole_sum(c * per + j)
        final_copy(own_rows(c), pl.ds(0, d)).start()

    def finish_last(j):
        p = last * per + j
        cross(pl.ds(p, 1), last + j).wait_recv()
        whole_sum(p)
        final_copy(*piece_of(p)).start()

    def hidden(r, lo, hi):
        for t in range(lo, hi):
            f = pl.ds(t * TILE, TILE)
            dh = dot(dy_v[r, :], dw_down[f, :], NT)
            g = gate_v[r, f].astype(F32)
            u = up_v[r, f].astype(F32)
            g2 = g * g
            s = 0.5 + 0.5 * jnp.tanh(g * (C0 + (C0 * C1) * g2))
            gelu = g * s
            slope = s + (g * (s * (1.0 - s))) * (2.0 * C0 + (6.0 * C0 * C1) * g2)
            hid_v[r, f] = (gelu * u).astype(BF16)
            gate_v[r, f] = (dh * u * slope).astype(BF16)
            up_v[r, f] = (dh * gelu).astype(BF16)

    first = chunk_loads(0)
    first[0].start()
    down_load(0).start()
    first[1].start()
    first[2].start()
    for b in range(1, len(downs)):
        down_load(b).start(priority=1)

    barrier = pltpu.get_barrier_semaphore()
    for device in (mate, across):
        pl.semaphore_signal(barrier, inc=1, **to(device))

    @pl.loop(0, n)
    def _(c):
        for w in chunk_loads(c):
            w.wait()

        r = pl.ds(pl.multiple_of(c * CHUNK, CHUNK), CHUNK)

        @pl.when(c == 0)
        def _():
            for b, (lo, hi) in enumerate(downs):
                down_load(b).wait()
                for j in ((0,), (1,), (2, 3))[b]:
                    for w in weight_loads(j) if j else half_loads(0) + half_loads(1):
                        w.start()
                hidden(r, lo, hi)
            pl.semaphore_wait(barrier, 2)

        @pl.when(c > 0)
        def _():
            hidden(r, 0, ff // TILE)

        @pl.when(c + 1 < n)
        def _():
            for w in chunk_loads(c + 1):
                w.start()

        @pl.when(c > 1)
        def _():
            add_mate(per * c - 2)

        @pl.when(c > 0)
        def _():
            add_mate(per * c - 1)

        mine = own_rows(c)
        other = pl.ds(pl.multiple_of(c * CHUNK + (1 - core) * HALF, HALF), HALF)
        for j in range(per):
            p = per * c + j

            if j > 0:

                @pl.when(c == 0)
                def _():
                    for w in weight_loads(j):
                        w.wait()

            def rows_of(ref):
                return jnp.concatenate([ref[mine, :], ref[other, :]], axis=0)

            def put(term, f):
                keep[j, :, f] = term[:HALF]
                give[j, :, f] = term[HALF:].astype(BF16)

            def terms():
                lhs = jnp.concatenate([rows_of(gate_v), rows_of(up_v)], axis=1)
                for t in range(PIECE // TILE):
                    w = pl.ds(j * PIECE + t * TILE, TILE)
                    rhs = jnp.concatenate([dw_gate[w, :], dw_up[w, :]], axis=1)
                    put(dot(lhs, rhs, NT), pl.ds(t * TILE, TILE))
                give_copy(p).start()

            if j == 0:

                @pl.when(c == 0)
                def _():
                    for t in range(PIECE // TILE):
                        for w in half_loads(t):
                            w.wait()
                        f, swap, _ = half(t)
                        term = dot(rows_of(gate_v), dw_gate[f, :], NT)
                        put(term + dot(rows_of(up_v), dw_up[f, :], NT), f)
                        swap.start()
                    add_half(0)

                @pl.when(c > 0)
                def _():
                    give_copy(p - per).wait_send()
                    terms()

            else:

                @pl.when(c > 0)
                def _():
                    give_copy(p - per).wait_send()

                terms()

            if j == 1:

                @pl.when(c == 0)
                def _():
                    add_half(1)

            if j > 1:

                @pl.when(c == 0)
                def _():
                    add_mate(p - 1)

                @pl.when(c > 0)
                def _():
                    add_mate(p - 2)

        @pl.when(c == n - 2)
        def _():
            x_load(0).start()

        @pl.when((c > 2) & (lax.rem(c, 2) == 1))
        def _():
            finish_chunk((c - 3) // 2)

    for p in (pieces - 2, pieces - 1):
        add_mate(p)
    for p in range(pieces - per, pieces):
        give_copy(p).wait_send()
    tiles = d // TILE

    @pl.loop(0, tiles)
    def _(k):
        x_load(k).wait()

        @pl.when(k + 1 < tiles)
        def _():
            x_load(k + 1).start()

        r = pl.ds(pl.multiple_of(k * TILE, TILE), TILE)
        slot = lax.rem(k, 2)
        dw_gate[r, :] = dot(x_v[slot], gate_v[...], TN).astype(BF16)
        dw_up[r, :] = dot(x_v[slot], up_v[...], TN).astype(BF16)

        @pl.when(lax.rem(k, 4) == 1)
        def _():
            finish_chunk(3 + k // 4)

    @pl.loop(0, ff // TILE)
    def _(k):
        f = pl.ds(pl.multiple_of(k * TILE, TILE), TILE)
        for h in range(2):
            c = pl.ds(h * (d // 2), d // 2)
            dw_down[f, c] = dot(hid_v[:, f], dy_v[:, c], TN).astype(BF16)

        @pl.when(k == 1)
        def _():
            finish_chunk(5)

    finish_chunk(6)
    for j in range(per):
        finish_last(j)

    total = pltpu.make_async_remote_copy(got_c, got_x, send_x_sem, got_fin_sem, **to(across))
    total.wait_send()
    total = pltpu.make_async_remote_copy(got_x, got_x, fin_sem, got_fin_sem, **to(mate))
    total.wait()


def store(*refs):
    n = len(refs) // 2
    copies = []
    for i in range(n):
        step = refs[i].shape[0] // SPLIT
        for k in range(SPLIT):
            r = pl.ds(k * step, step)
            copies.append(pltpu.make_async_copy(refs[i].at[r], refs[n + i].at[r], refs[-1].at[i, k]))
    for c in copies:
        c.start()
    for c in copies:
        c.wait()


def backward(x, dy, gate, up, w_gate, w_up, w_down):
    rows, d = x.shape
    ff = gate.shape[1]
    per = d // PIECE
    pieces = per * rows // CHUNK
    hbm = pl.BlockSpec(memory_space=pl.ANY)
    sem = pltpu.SemaphoreType.DMA
    parts = pl.pallas_call(
        kernel,
        out_shape=tuple(pltpu.VMEM(s, BF16) for s in ((rows, d), (d, ff), (d, ff), (ff, d))),
        in_specs=[hbm] * 7,
        out_specs=(pl.BlockSpec(memory_space=pltpu.VMEM),) * 4,
        scratch_shapes=[
            pltpu.VMEM((rows, d), BF16),
            pltpu.VMEM((rows, ff), BF16),
            pltpu.VMEM((rows, ff), BF16),
            pltpu.VMEM((rows, ff), BF16),
            pltpu.VMEM((pieces, HALF, PIECE), BF16),
            pltpu.VMEM((pieces, HALF, PIECE), BF16),
            pltpu.VMEM((per, HALF, PIECE), F32),
            pltpu.VMEM((per, HALF, PIECE), BF16),
            pltpu.VMEM((2, rows, TILE), BF16),
            sem((4, per)),
            sem((3, 2)),
            sem((2,)),
            sem((per,)),
            sem((RING + 1,)),
            sem,
            sem((rows // CHUNK - 1 + per,)),
            sem,
            sem,
        ],
        compiler_params=pltpu.CompilerParams(
            collective_id=0,
            has_side_effects=True,
            vmem_limit_bytes=39 * 2**20,
        ),
        cost_estimate=pl.CostEstimate(
            flops=12 * rows * d * ff, bytes_accessed=64 * 2**20, transcendentals=rows * ff
        ),
        name="mlp_backward",
    )(x, dy, gate, up, w_gate, w_up, w_down)
    return pl.pallas_call(
        store,
        out_shape=tuple(pltpu.HBM(p.shape, p.dtype) for p in parts),
        in_specs=[pl.BlockSpec(memory_space=pltpu.VMEM)] * len(parts),
        out_specs=(pl.BlockSpec(memory_space=pltpu.HBM),) * len(parts),
        scratch_shapes=[sem((len(parts), SPLIT))],
        compiler_params=pltpu.CompilerParams(vmem_limit_bytes=2**20),
        name="store",
    )(*parts)


def solution(mesh):
    tokens, columns, down = P("dp", None), P(None, "tp"), P("tp", None)
    return jax.shard_map(
        backward,
        mesh=mesh,
        in_specs=(tokens, tokens, P("dp", "tp"), P("dp", "tp"), columns, columns, down),
        out_specs=(tokens, P("dp", "tp"), P("dp", "tp"), P(("dp", "tp"), None)),
        check_vma=False,
    )
```

```python
import functools

import jax
import jax.numpy as jnp
from jax import lax
from jax.experimental import pallas as pl
from jax.experimental.pallas import tpu as pltpu
from jax.sharding import PartitionSpec as P

MESH = pl.DeviceIdType.MESH
NT = (((1,), (1,)), ((), ()))
TN = (((0,), (0,)), ((), ()))
BF16, F32 = jnp.bfloat16, jnp.float32

CHUNK = 256
HALF = CHUNK // 2
TILE = 256
PIECE = 512
RING = 6
SPLIT = 2
C0 = 0.7978845608028654
C1 = 0.044715


def dot(a, b, dims):
    return lax.dot_general(a, b, dims, preferred_element_type=F32)


def kernel(
    x, dy, gate, up, w_gate, w_up, w_down,
    dx, dw_gate, dw_up, dw_down,
    dy_v, gate_v, up_v, hid_v, got_x, got_c, keep, give, x_v,
    w_sem, in_sem, x_sem, give_sem, got_c_sem, send_x_sem, got_x_sem, fin_sem, got_fin_sem,
):
    rows, d = dx.shape
    ff = dw_gate.shape[1]
    n = rows // CHUNK
    per = d // PIECE
    pieces = per * n
    downs = [(0, 1), (1, 3), (3, 5)]
    last = n - 1
    me = lax.axis_index("tp")
    core = lax.rem(me, 2)
    mate = me + 1 - 2 * core
    across = lax.rem(me + 2, 4)

    def load(src, dst, sem):
        return pltpu.make_async_copy(src, dst, sem)

    def chunk_loads(c):
        r = pl.ds(pl.multiple_of(c * CHUNK, CHUNK), CHUNK)
        return [
            load(dy.at[r], dy_v.at[r], in_sem.at[0, lax.rem(c, 2)]),
            load(gate.at[r], gate_v.at[r], in_sem.at[1, lax.rem(c, 2)]),
            load(up.at[r], up_v.at[r], in_sem.at[2, lax.rem(c, 2)]),
        ]

    def weight_loads(j):
        r = pl.ds(j * PIECE, PIECE)
        return [
            load(w_gate.at[r], dw_gate.at[r], w_sem.at[j]),
            load(w_up.at[r], dw_up.at[r], w_sem.at[per + j]),
        ]

    def half_loads(t):
        r = pl.ds(t * TILE, TILE)
        return [
            load(w_gate.at[r], dw_gate.at[r], w_sem.at[t * (2 * per + 3)]),
            load(w_up.at[r], dw_up.at[r], w_sem.at[per + t * (per + 4)]),
        ]

    def down_load(b):
        lo, hi = downs[b]
        r = pl.ds(lo * TILE, (hi - lo) * TILE)
        return load(w_down.at[r], dw_down.at[r], w_sem.at[2 * per + b])

    def x_load(k):
        c = pl.ds(pl.multiple_of(k * TILE, TILE), TILE)
        slot = lax.rem(k, 2)
        return load(x.at[:, c], x_v.at[slot], x_sem.at[slot])

    def to(device):
        return dict(device_id={"tp": device}, device_id_type=MESH)

    def own_rows(c):
        return pl.ds(pl.multiple_of(c * CHUNK + core * HALF, HALF), HALF)

    def piece_of(p):
        c, j = p // per, lax.rem(p, per)
        return own_rows(c), pl.ds(pl.multiple_of(j * PIECE, PIECE), PIECE)

    def give_copy(p):
        return pltpu.make_async_remote_copy(
            give.at[lax.rem(p, per)],
            got_c.at[p],
            give_sem.at[lax.rem(p, per)],
            got_c_sem.at[lax.rem(p, RING)],
            **to(mate),
        )

    def cross(refs, slot):
        return pltpu.make_async_remote_copy(
            got_c.at[refs], got_x.at[refs], send_x_sem, got_x_sem.at[slot], **to(across)
        )

    def final_copy(r, c):
        return pltpu.make_async_remote_copy(
            dx.at[r, c], dx.at[r, c], fin_sem, got_fin_sem, **to(mate)
        )

    def add_mate(p):
        give_copy(p).wait_recv()
        got_c[p] = (keep[lax.rem(p, per)] + got_c[p].astype(F32)).astype(BF16)
        slot = jnp.where(p < last * per, p // per, p - last * (per - 1))
        cross(pl.ds(p, 1), slot).start()

    def half(t):
        f = pl.ds(t * TILE, TILE)
        swap = pltpu.make_async_remote_copy(
            give.at[0, :, f], got_c.at[0, :, f], give_sem.at[0], got_c_sem.at[t * RING], **to(mate)
        )
        away = pltpu.make_async_remote_copy(
            got_c.at[0, :, f], got_x.at[0, :, f], send_x_sem, got_x_sem.at[0], **to(across)
        )
        return f, swap, away

    def add_half(t):
        f, swap, away = half(t)
        swap.wait_recv()
        got_c[0, :, f] = (keep[0, :, f] + got_c[0, :, f].astype(F32)).astype(BF16)
        away.start()

    def whole_sum(p):
        r, c = piece_of(p)
        dx[r, c] = (got_c[p].astype(F32) + got_x[p].astype(F32)).astype(BF16)

    def finish_chunk(c):
        cross(pl.ds(pl.multiple_of(c * per, per), per), c).wait_recv()
        for j in range(per):
            whole_sum(c * per + j)
        final_copy(own_rows(c), pl.ds(0, d)).start()

    def finish_last(j):
        p = last * per + j
        cross(pl.ds(p, 1), last + j).wait_recv()
        whole_sum(p)
        final_copy(*piece_of(p)).start()

    def hidden(r, lo, hi):
        for t in range(lo, hi):
            f = pl.ds(t * TILE, TILE)
            dh = dot(dy_v[r, :], dw_down[f, :], NT)
            g = gate_v[r, f].astype(F32)
            u = up_v[r, f].astype(F32)
            g2 = g * g
            s = 0.5 + 0.5 * jnp.tanh(g * (C0 + (C0 * C1) * g2))
            gelu = g * s
            slope = s + (g * (s * (1.0 - s))) * (2.0 * C0 + (6.0 * C0 * C1) * g2)
            hid_v[r, f] = (gelu * u).astype(BF16)
            gate_v[r, f] = (dh * u * slope).astype(BF16)
            up_v[r, f] = (dh * gelu).astype(BF16)

    first = chunk_loads(0)
    first[0].start()
    down_load(0).start()
    first[1].start()
    first[2].start()
    for b in range(1, len(downs)):
        down_load(b).start(priority=1)

    barrier = pltpu.get_barrier_semaphore()
    for device in (mate, across):
        pl.semaphore_signal(barrier, inc=1, **to(device))

    @pl.loop(0, n)
    def _(c):
        for w in chunk_loads(c):
            w.wait()

        r = pl.ds(pl.multiple_of(c * CHUNK, CHUNK), CHUNK)

        mine = own_rows(c)
        other = pl.ds(pl.multiple_of(c * CHUNK + (1 - core) * HALF, HALF), HALF)

        def rows_of(ref):
            return jnp.concatenate([ref[mine, :], ref[other, :]], axis=0)

        def half_terms(t):
            f, swap, _ = half(t)
            term = dot(rows_of(gate_v), dw_gate[f, :], NT) + dot(rows_of(up_v), dw_up[f, :], NT)
            keep[0, :, f] = term[:HALF]
            give[0, :, f] = term[HALF:].astype(BF16)
            swap.start()

        @pl.when(c == 0)
        def _():
            for b, (lo, hi) in enumerate(downs):
                down_load(b).wait()
                for j in ((0,), (1,), (2, 3))[b]:
                    for w in weight_loads(j) if j else half_loads(0) + half_loads(1):
                        w.start()
                if hi == ff // TILE:
                    pl.semaphore_wait(barrier, 2)
                    for w in half_loads(0):
                        w.wait()
                hidden(r, lo, hi)
            half_terms(0)

        @pl.when(c > 0)
        def _():
            hidden(r, 0, ff // TILE)

        @pl.when(c + 1 < n)
        def _():
            for w in chunk_loads(c + 1):
                w.start()

        @pl.when(c > 1)
        def _():
            add_mate(per * c - 2)

        @pl.when(c > 0)
        def _():
            add_mate(per * c - 1)

        for j in range(per):
            p = per * c + j

            if j > 0:

                @pl.when(c == 0)
                def _():
                    for w in weight_loads(j):
                        w.wait()

            def put(term, f):
                keep[j, :, f] = term[:HALF]
                give[j, :, f] = term[HALF:].astype(BF16)

            def terms():
                lhs = jnp.concatenate([rows_of(gate_v), rows_of(up_v)], axis=1)
                for t in range(PIECE // TILE):
                    w = pl.ds(j * PIECE + t * TILE, TILE)
                    rhs = jnp.concatenate([dw_gate[w, :], dw_up[w, :]], axis=1)
                    put(dot(lhs, rhs, NT), pl.ds(t * TILE, TILE))
                give_copy(p).start()

            if j == 0:

                @pl.when(c == 0)
                def _():
                    for w in half_loads(1):
                        w.wait()
                    half_terms(1)
                    add_half(0)

                @pl.when(c > 0)
                def _():
                    give_copy(p - per).wait_send()
                    terms()

            else:

                @pl.when(c > 0)
                def _():
                    give_copy(p - per).wait_send()

                terms()

            if j == 1:

                @pl.when(c == 0)
                def _():
                    add_half(1)

            if j > 1:

                @pl.when(c == 0)
                def _():
                    add_mate(p - 1)

                @pl.when(c > 0)
                def _():
                    add_mate(p - 2)

        @pl.when(c == n - 2)
        def _():
            x_load(0).start()

        @pl.when((c > 2) & (lax.rem(c, 2) == 1))
        def _():
            finish_chunk((c - 3) // 2)

    for p in (pieces - 2, pieces - 1):
        add_mate(p)
    for p in range(pieces - per, pieces):
        give_copy(p).wait_send()
    tiles = d // TILE

    @pl.loop(0, tiles)
    def _(k):
        x_load(k).wait()

        @pl.when(k + 1 < tiles)
        def _():
            x_load(k + 1).start()

        r = pl.ds(pl.multiple_of(k * TILE, TILE), TILE)
        slot = lax.rem(k, 2)
        dw_gate[r, :] = dot(x_v[slot], gate_v[...], TN).astype(BF16)
        dw_up[r, :] = dot(x_v[slot], up_v[...], TN).astype(BF16)

        @pl.when(lax.rem(k, 4) == 1)
        def _():
            finish_chunk(3 + k // 4)

    @pl.loop(0, ff // TILE)
    def _(k):
        f = pl.ds(pl.multiple_of(k * TILE, TILE), TILE)
        for h in range(2):
            c = pl.ds(h * (d // 2), d // 2)
            dw_down[f, c] = dot(hid_v[:, f], dy_v[:, c], TN).astype(BF16)

        @pl.when(k == 1)
        def _():
            finish_chunk(5)

    finish_chunk(6)
    for j in range(per):
        finish_last(j)

    total = pltpu.make_async_remote_copy(got_c, got_x, send_x_sem, got_fin_sem, **to(across))
    total.wait_send()
    total = pltpu.make_async_remote_copy(got_x, got_x, fin_sem, got_fin_sem, **to(mate))
    total.wait()


def store(*refs):
    n = len(refs) // 2
    copies = []
    for i in range(n):
        step = refs[i].shape[0] // SPLIT
        for k in range(SPLIT):
            r = pl.ds(k * step, step)
            copies.append(pltpu.make_async_copy(refs[i].at[r], refs[n + i].at[r], refs[-1].at[i, k]))
    for c in copies:
        c.start()
    for c in copies:
        c.wait()


def backward(x, dy, gate, up, w_gate, w_up, w_down):
    rows, d = x.shape
    ff = gate.shape[1]
    per = d // PIECE
    pieces = per * rows // CHUNK
    hbm = pl.BlockSpec(memory_space=pl.ANY)
    sem = pltpu.SemaphoreType.DMA
    parts = pl.pallas_call(
        kernel,
        out_shape=tuple(pltpu.VMEM(s, BF16) for s in ((rows, d), (d, ff), (d, ff), (ff, d))),
        in_specs=[hbm] * 7,
        out_specs=(pl.BlockSpec(memory_space=pltpu.VMEM),) * 4,
        scratch_shapes=[
            pltpu.VMEM((rows, d), BF16),
            pltpu.VMEM((rows, ff), BF16),
            pltpu.VMEM((rows, ff), BF16),
            pltpu.VMEM((rows, ff), BF16),
            pltpu.VMEM((pieces, HALF, PIECE), BF16),
            pltpu.VMEM((pieces, HALF, PIECE), BF16),
            pltpu.VMEM((per, HALF, PIECE), F32),
            pltpu.VMEM((per, HALF, PIECE), BF16),
            pltpu.VMEM((2, rows, TILE), BF16),
            sem((2 * per + 5,)),
            sem((3, 2)),
            sem((2,)),
            sem((per,)),
            sem((RING + 1,)),
            sem,
            sem((rows // CHUNK - 1 + per,)),
            sem,
            sem,
        ],
        compiler_params=pltpu.CompilerParams(
            collective_id=0,
            has_side_effects=True,
            vmem_limit_bytes=39 * 2**20,
        ),
        cost_estimate=pl.CostEstimate(
            flops=12 * rows * d * ff, bytes_accessed=64 * 2**20, transcendentals=rows * ff
        ),
        name="mlp_backward",
    )(x, dy, gate, up, w_gate, w_up, w_down)
    return pl.pallas_call(
        store,
        out_shape=tuple(pltpu.HBM(p.shape, p.dtype) for p in parts),
        in_specs=[pl.BlockSpec(memory_space=pltpu.VMEM)] * len(parts),
        out_specs=(pl.BlockSpec(memory_space=pltpu.HBM),) * len(parts),
        scratch_shapes=[sem((len(parts), SPLIT))],
        compiler_params=pltpu.CompilerParams(vmem_limit_bytes=2**20),
        name="store",
    )(*parts)


def solution(mesh):
    tokens, columns, down = P("dp", None), P(None, "tp"), P("tp", None)
    return jax.shard_map(
        backward,
        mesh=mesh,
        in_specs=(tokens, tokens, P("dp", "tp"), P("dp", "tp"), columns, columns, down),
        out_specs=(tokens, P("dp", "tp"), P("dp", "tp"), P(("dp", "tp"), None)),
        check_vma=False,
    )
```
